16 devices in a mesh: dp: 4 (over y, z, core), tp: 4 (over x).
Axes of the slice: x: 4, y: 2, z: 1, core: 2. Of those that a mesh axis runs over, the one named last changes fastest.
The devices are a block of a 4x4x8 slice.
Arguments:
- x: bfloat16 [512, 5120], P('dp'), parts along dimension 0
- w_gate: bfloat16 [5120, 25600], P(None, 'tp')
- w_up: bfloat16 [5120, 25600], P(None, 'tp')
- w_down: bfloat16 [25600, 5120], P('tp')
Outputs:
- output: bfloat16 [512, 5120], P('dp'), parts along dimension 0
There are 4 independent parts. The reference program is written for one: setup_inputs(seed, part) draws one part's arguments, and reference() takes and returns one part's arrays. A program takes and returns all parts, laid end to end along the dimension named above; an argument that names none is the same for every part.
All inputs are finite; a program needn't handle non-finite values.
Results may differ from the reference program's by a relative error of at most 0.016.
Values are sent between devices in bfloat16 or wider.
A program may use at most 768 MiB of HBM per device.

```python
import jax
import jax.numpy as jnp

ROWS = 128
D = 5120
FF = 25600


def setup_inputs(seed: int = 0, part: int = 0) -> dict:
    kx, kg, ku, kd = jax.random.split(jax.random.key(seed), 4)
    drawn = {
        "x": jax.random.normal(jax.random.fold_in(kx, part), (ROWS, D), jnp.float32),
        "w_gate": jax.random.normal(kg, (D, FF), jnp.float32) * D**-0.5,
        "w_up": jax.random.normal(ku, (D, FF), jnp.float32) * D**-0.5,
        "w_down": jax.random.normal(kd, (FF, D), jnp.float32) * FF**-0.5,
    }
    return {k: v.astype(jnp.bfloat16) for k, v in drawn.items()}


def reference(x, w_gate, w_up, w_down):
    gate = jnp.dot(x, w_gate, preferred_element_type=jnp.float32)
    up = jnp.dot(x, w_up, preferred_element_type=jnp.float32)
    hidden = (jax.nn.silu(gate) * up).astype(jnp.bfloat16)
    return jnp.dot(hidden, w_down, preferred_element_type=jnp.float32).astype(jnp.bfloat16)
```

```python
import functools

import jax
import jax.numpy as jnp
from jax import lax
from jax.experimental import pallas as pl
from jax.experimental.pallas import tpu as pltpu
from jax.sharding import PartitionSpec as P

MESH = pl.DeviceIdType.MESH
SLOTS = 8
WIDE = 512
XCUT = 4


def kernel(x, wg, wu, wd, y, xs, h, slots, acc, dsend, drecv, term, s1, r1, s2, r2, wsem, xsem, dsem, rsem, gsem):
    rows, d = x.shape
    half = wg.shape[1] // 2
    unit = WIDE // 2
    first = half % unit
    steps = half // unit + 1
    chunks = d // WIDE
    piece = WIDE // 4
    top = rows // 2

    dp, tp = lax.axis_index("dp"), lax.axis_index("tp")
    core = lax.rem(dp, 2)
    other = {"dp": dp + 1 - 2 * core}
    right_at, left_at, far_at = lax.rem(tp + 1, 4), lax.rem(tp + 3, 4), lax.rem(tp + 2, 4)
    right, left = {"tp": right_at}, {"tp": left_at}
    base = core * half

    def gate_up(step, width):
        slot = lax.rem(step, SLOTS)
        at = base if width == first else base + first + (step - 1) * unit
        cols = pl.ds(pl.multiple_of(at, 128), width)
        return [
            pltpu.make_async_copy(w.at[:, cols], slots.at[slot, :, pl.ds(k * width, width)], wsem.at[slot, k])
            for k, w in enumerate((wg, wu))
        ]

    def down(chunk):
        slot = lax.rem(chunk + steps, SLOTS)
        cols = pl.ds(pl.multiple_of(chunk * WIDE, 128), WIDE)
        return pltpu.make_async_copy(
            wd.at[pl.ds(pl.multiple_of(base, 128), half), cols], slots.at[slot, pl.ds(0, half), :], wsem.at[slot, 0]
        )

    def refill(step):
        @pl.when(step < steps)
        def _():
            for c in gate_up(step, unit):
                c.start()

        @pl.when(jnp.logical_and(step >= steps, step < steps + chunks))
        def _():
            down(step - steps).start()

    xw = d // XCUT

    def x_in(k):
        cols = pl.ds(k * xw, xw)
        return pltpu.make_async_copy(x.at[:, cols], xs.at[pl.ds(0, rows), cols], xsem.at[0, k])

    def x_out(k):
        cols = pl.ds(k * xw, xw)
        return pltpu.make_async_remote_copy(
            src_ref=xs.at[pl.ds(0, rows), cols],
            dst_ref=xs.at[pl.ds(rows, rows), cols],
            send_sem=xsem.at[1, k],
            recv_sem=xsem.at[2, k],
            device_id=other,
            device_id_type=MESH,
        )

    for k in range(XCUT):
        x_in(k).start()
    for c in gate_up(0, first):
        c.start()
    for s in range(1, SLOTS):
        for c in gate_up(s, unit):
            c.start()

    barrier = pltpu.get_barrier_semaphore()
    for who in (other, right, left):
        pl.semaphore_signal(barrier, inc=1, device_id=who, device_id_type=MESH)
    pl.semaphore_wait(barrier, 3)

    for k in range(XCUT):
        x_in(k).wait()
        x_out(k).start()
    for k in range(XCUT):
        x_out(k).wait_recv()

    def hidden(step, width, at):
        slot = lax.rem(step, SLOTS)
        for c in gate_up(step, width):
            c.wait()
        both = jnp.dot(xs[...], slots[slot, :, : 2 * width], preferred_element_type=jnp.float32)
        h[:, pl.ds(at, width)] = (jax.nn.silu(both[:, :width]) * both[:, width:]).astype(h.dtype)
        refill(step + SLOTS)

    hidden(0, first, 0)

    @pl.loop(1, steps)
    def _(s):
        hidden(s, unit, pl.multiple_of(first + (s - 1) * unit, 128))

    def send(src, dst, sems, k, j, who):
        return pltpu.make_async_remote_copy(
            src_ref=src, dst_ref=dst, send_sem=sems.at[0, k, j], recv_sem=sems.at[1, k, j], device_id=who, device_id_type=MESH
        )

    def die(j):
        return send(dsend.at[j], drecv.at[j], dsem, 0, j, other)

    def rs1(j, k):
        return send(s1.at[k, j], r1.at[k, j], rsem, k, j, (right, left)[k])

    def rs2(j, k):
        return send(s2.at[k, j], r2.at[k, j], rsem, 2 + k, j, (right, left)[k])

    def block(j, at, k=None):
        span = pl.ds(0, rows) if k is None else pl.ds(k * top, top)
        return y.at[span, pl.ds(pl.multiple_of(j * WIDE + at * piece, 128), piece)]

    def ag1(j, k):
        return send(block(j, tp), block(j, tp), gsem, k, j, (right, left)[k])

    def ag1_in(j, k):
        at = (left_at, right_at)[k]
        return send(block(j, at), block(j, at), gsem, k, j, (right, left)[k])

    def ag2(j, k):
        at = (left_at, right_at)[k]
        return send(block(j, at, k), block(j, at, k), gsem, 2 + k, j, (right, left)[k])

    def ag2_in(j, k):
        return send(block(j, far_at, k), block(j, far_at, k), gsem, 2 + k, j, (right, left)[k])

    def part(j, at, k):
        return term[j, pl.ds(k * top, top), pl.ds(pl.multiple_of(at * piece, 128), piece)]

    def chip_sum(j):
        die(j).wait_recv()
        term[j] = acc[lax.rem(j, 2)] + drecv[j].astype(jnp.float32)
        for k in range(2):
            s1[k, j, 0] = part(j, far_at, k).astype(s1.dtype)
            s1[k, j, 1] = part(j, (right_at, left_at)[k], 1 - k).astype(s1.dtype)
            rs1(j, k).start()

    def pass_on(j):
        for k in range(2):
            rs1(j, k).wait_recv()
            s2[k, j] = (part(j, (right_at, left_at)[k], k) + r1[k, j, 0].astype(jnp.float32)).astype(s2.dtype)
            rs2(j, k).start()

    def finish(j):
        for k in range(2):
            rs2(j, k).wait_recv()
            total = part(j, tp, k) + r2[k, j].astype(jnp.float32) + r1[1 - k, j, 1].astype(jnp.float32)
            block(j, tp, k)[...] = total.astype(y.dtype)
        for k in range(2):
            ag1(j, k).start()

    def forward(j):
        for k in range(2):
            ag1_in(j, k).wait_recv()
            ag2(j, k).start()

    @pl.loop(0, chunks)
    def _(j):
        slot = lax.rem(j + steps, SLOTS)
        down(j).wait()
        out = jnp.dot(h[...], slots[slot, :half, :], preferred_element_type=jnp.float32)
        acc[lax.rem(j, 2)] = out[:rows]
        dsend[j] = out[rows:].astype(dsend.dtype)
        die(j).start()
        refill(j + steps + SLOTS)

        @pl.when(j >= 1)
        def _():
            chip_sum(j - 1)

        @pl.when(j >= 2)
        def _():
            pass_on(j - 2)

    chip_sum(chunks - 1)
    pass_on(chunks - 2)
    pass_on(chunks - 1)

    @pl.loop(0, chunks)
    def _(j):
        finish(j)

    @pl.loop(0, chunks)
    def _(j):
        forward(j)

    @pl.loop(0, chunks)
    def _(j):
        for k in range(2):
            ag2_in(j, k).wait_recv()

    for k in range(XCUT):
        x_out(k).wait_send()

    @pl.loop(0, chunks)
    def _(j):
        die(j).wait_send()
        for k in range(2):
            rs1(j, k).wait_send()
            rs2(j, k).wait_send()
            ag1(j, k).wait_send()
            ag2(j, k).wait_send()


def solution(mesh):
    assert mesh.shape["tp"] == 4 and mesh.shape["dp"] % 2 == 0

    def step(x, w_gate, w_up, w_down):
        rows, d = x.shape
        half = w_gate.shape[1] // 2
        chunks, piece, top = d // WIDE, WIDE // 4, rows // 2
        dma = pltpu.SemaphoreType.DMA
        return pl.pallas_call(
            kernel,
            out_shape=jax.ShapeDtypeStruct((rows, d), jnp.bfloat16),
            in_specs=[pl.BlockSpec(memory_space=pl.ANY)] * 4,
            out_specs=pl.BlockSpec(memory_space=pltpu.VMEM),
            scratch_shapes=[
                pltpu.VMEM((2 * rows, d), jnp.bfloat16),
                pltpu.VMEM((2 * rows, half), jnp.bfloat16),
                pltpu.VMEM((SLOTS, d, WIDE), jnp.bfloat16),
                pltpu.VMEM((2, rows, WIDE), jnp.float32),
                pltpu.VMEM((chunks, rows, WIDE), jnp.bfloat16),
                pltpu.VMEM((chunks, rows, WIDE), jnp.bfloat16),
                pltpu.VMEM((chunks, rows, WIDE), jnp.float32),
                pltpu.VMEM((2, chunks, 2, top, piece), jnp.bfloat16),
                pltpu.VMEM((2, chunks, 2, top, piece), jnp.bfloat16),
                pltpu.VMEM((2, chunks, top, piece), jnp.bfloat16),
                pltpu.VMEM((2, chunks, top, piece), jnp.bfloat16),
                dma((SLOTS, 2)),
                dma((3, XCUT)),
                dma((2, 1, chunks)),
                dma((2, 4, chunks)),
                dma((2, 4, chunks)),
            ],
            compiler_params=pltpu.CompilerParams(
                collective_id=0, has_side_effects=True, vmem_limit_bytes=67043328
            ),
        )(x, w_gate, w_up, w_down)

    return jax.shard_map(
        step,
        mesh=mesh,
        in_specs=(P("dp", None), P(None, "tp"), P(None, "tp"), P("tp", None)),
        out_specs=P("dp", None),
        check_vma=False,
    )
```

```python
import functools

import jax
import jax.numpy as jnp
from jax import lax
from jax.experimental import pallas as pl
from jax.experimental.pallas import tpu as pltpu
from jax.sharding import PartitionSpec as P

MESH = pl.DeviceIdType.MESH
SLOTS = 8
WIDE = 512
XCUT = 4
EARLY = 2
LAG = 4


def kernel(x, wg, wu, wd, y, xs, h, slots, acc, dsend, drecv, term, s1, r1, s2, r2, wsem, xsem, dsem, rsem, gsem):
    rows, d = x.shape
    half = wg.shape[1] // 2
    unit = WIDE // 2
    first = half % unit
    steps = half // unit + 1
    chunks = d // WIDE
    piece = WIDE // 4
    top = rows // 2

    dp, tp = lax.axis_index("dp"), lax.axis_index("tp")
    core = lax.rem(dp, 2)
    other = {"dp": dp + 1 - 2 * core}
    right_at, left_at, far_at = lax.rem(tp + 1, 4), lax.rem(tp + 3, 4), lax.rem(tp + 2, 4)
    right, left = {"tp": right_at}, {"tp": left_at}
    base = core * half

    def gate_up(step, width):
        slot = lax.rem(step, SLOTS)
        at = base if width == first else base + first + (step - 1) * unit
        cols = pl.ds(pl.multiple_of(at, 128), width)
        return [
            pltpu.make_async_copy(w.at[:, cols], slots.at[slot, :, pl.ds(k * width, width)], wsem.at[slot, k])
            for k, w in enumerate((wg, wu))
        ]

    def down(chunk):
        slot = lax.rem(chunk + steps, SLOTS)
        cols = pl.ds(pl.multiple_of(chunk * WIDE, 128), WIDE)
        return pltpu.make_async_copy(
            wd.at[pl.ds(pl.multiple_of(base, 128), half), cols], slots.at[slot, pl.ds(0, half), :], wsem.at[slot, 0]
        )

    def refill(step):
        @pl.when(step < steps)
        def _():
            for c in gate_up(step, unit):
                c.start()

        @pl.when(jnp.logical_and(step >= steps, step < steps + chunks))
        def _():
            down(step - steps).start()

    xw = d // XCUT

    def x_in(k):
        cols = pl.ds(k * xw, xw)
        return pltpu.make_async_copy(x.at[:, cols], xs.at[pl.ds(0, rows), cols], xsem.at[0, k])

    def x_out(k):
        cols = pl.ds(k * xw, xw)
        return pltpu.make_async_remote_copy(
            src_ref=xs.at[pl.ds(0, rows), cols],
            dst_ref=xs.at[pl.ds(rows, rows), cols],
            send_sem=xsem.at[1, k],
            recv_sem=xsem.at[2, k],
            device_id=other,
            device_id_type=MESH,
        )

    barrier = pltpu.get_barrier_semaphore()
    for who in (other, right, left):
        pl.semaphore_signal(barrier, inc=1, device_id=who, device_id_type=MESH)
    for k in range(XCUT):
        x_in(k).start()
    for s in range(EARLY):
        for c in gate_up(s, unit if s else first):
            c.start()
    pl.semaphore_wait(barrier, 3)

    for k in range(XCUT):
        x_in(k).wait()
        x_out(k).start()
    for s in range(EARLY, SLOTS):
        for c in gate_up(s, unit):
            c.start()
    for k in range(XCUT):
        x_out(k).wait_recv()

    def hidden(step, width, at):
        slot = lax.rem(step, SLOTS)
        for c in gate_up(step, width):
            c.wait()
        both = jnp.dot(xs[...], slots[slot, :, : 2 * width], preferred_element_type=jnp.float32)
        h[:, pl.ds(at, width)] = (jax.nn.silu(both[:, :width]) * both[:, width:]).astype(h.dtype)
        refill(step + SLOTS)

    hidden(0, first, 0)

    @pl.loop(1, steps)
    def _(s):
        hidden(s, unit, pl.multiple_of(first + (s - 1) * unit, 128))

    def send(src, dst, sems, k, j, who):
        return pltpu.make_async_remote_copy(
            src_ref=src, dst_ref=dst, send_sem=sems.at[0, k, j], recv_sem=sems.at[1, k, j], device_id=who, device_id_type=MESH
        )

    def die(j):
        return send(dsend.at[j], drecv.at[j], dsem, 0, j, other)

    def rs1(j, k):
        return send(s1.at[k, j], r1.at[k, j], rsem, k, j, (right, left)[k])

    def rs2(j, k):
        return send(s2.at[k, j], r2.at[k, j], rsem, 2 + k, j, (right, left)[k])

    def block(j, at, k=None):
        span = pl.ds(0, rows) if k is None else pl.ds(k * top, top)
        return y.at[span, pl.ds(pl.multiple_of(j * WIDE + at * piece, 128), piece)]

    def ag1(j, k):
        return send(block(j, tp), block(j, tp), gsem, k, j, (right, left)[k])

    def ag1_in(j, k):
        at = (left_at, right_at)[k]
        return send(block(j, at), block(j, at), gsem, k, j, (right, left)[k])

    def ag2(j, k):
        at = (left_at, right_at)[k]
        return send(block(j, at, k), block(j, at, k), gsem, 2 + k, j, (right, left)[k])

    def ag2_in(j, k):
        return send(block(j, far_at, k), block(j, far_at, k), gsem, 2 + k, j, (right, left)[k])

    def part(j, at, k):
        return term[j, pl.ds(k * top, top), pl.ds(pl.multiple_of(at * piece, 128), piece)]

    def chip_sum(j):
        die(j).wait_recv()
        term[j] = acc[lax.rem(j, 2)] + drecv[j].astype(jnp.float32)
        for k in range(2):
            s1[k, j, 0] = part(j, far_at, k).astype(s1.dtype)
            s1[k, j, 1] = part(j, (right_at, left_at)[k], 1 - k).astype(s1.dtype)
            rs1(j, k).start()

    def pass_on(j):
        for k in range(2):
            rs1(j, k).wait_recv()
            s2[k, j] = (part(j, (right_at, left_at)[k], k) + r1[k, j, 0].astype(jnp.float32)).astype(s2.dtype)
            rs2(j, k).start()

    def finish(j):
        for k in range(2):
            rs2(j, k).wait_recv()
            total = part(j, tp, k) + r2[k, j].astype(jnp.float32) + r1[1 - k, j, 1].astype(jnp.float32)
            block(j, tp, k)[...] = total.astype(y.dtype)
        for k in range(2):
            ag1(j, k).start()

    def forward(j):
        for k in range(2):
            ag1_in(j, k).wait_recv()
            ag2(j, k).start()

    @pl.loop(0, chunks)
    def _(j):
        slot = lax.rem(j + steps, SLOTS)
        down(j).wait()
        out = jnp.dot(h[...], slots[slot, :half, :], preferred_element_type=jnp.float32)
        acc[lax.rem(j, 2)] = out[:rows]
        dsend[j] = out[rows:].astype(dsend.dtype)
        die(j).start()
        refill(j + steps + SLOTS)

        @pl.when(j >= 1)
        def _():
            chip_sum(j - 1)

        @pl.when(j >= LAG)
        def _():
            pass_on(j - LAG)

    chip_sum(chunks - 1)

    @pl.loop(chunks - LAG, chunks)
    def _(j):
        pass_on(j)

    @pl.loop(0, chunks)
    def _(j):
        finish(j)

    @pl.loop(0, chunks)
    def _(j):
        forward(j)

    @pl.loop(0, chunks)
    def _(j):
        for k in range(2):
            ag2_in(j, k).wait_recv()

    for k in range(XCUT):
        x_out(k).wait_send()

    @pl.loop(0, chunks)
    def _(j):
        die(j).wait_send()
        for k in range(2):
            rs1(j, k).wait_send()
            rs2(j, k).wait_send()
            ag1(j, k).wait_send()
            ag2(j, k).wait_send()


def solution(mesh):
    assert mesh.shape["tp"] == 4 and mesh.shape["dp"] % 2 == 0

    def step(x, w_gate, w_up, w_down):
        rows, d = x.shape
        half = w_gate.shape[1] // 2
        chunks, piece, top = d // WIDE, WIDE // 4, rows // 2
        dma = pltpu.SemaphoreType.DMA
        return pl.pallas_call(
            kernel,
            out_shape=pltpu.VMEM((rows, d), jnp.bfloat16),
            in_specs=[pl.BlockSpec(memory_space=pl.ANY)] * 4,
            out_specs=pl.BlockSpec(memory_space=pltpu.VMEM),
            scratch_shapes=[
                pltpu.VMEM((2 * rows, d), jnp.bfloat16),
                pltpu.VMEM((2 * rows, half), jnp.bfloat16),
                pltpu.VMEM((SLOTS, d, WIDE), jnp.bfloat16),
                pltpu.VMEM((2, rows, WIDE), jnp.float32),
                pltpu.VMEM((chunks, rows, WIDE), jnp.bfloat16),
                pltpu.VMEM((chunks, rows, WIDE), jnp.bfloat16),
                pltpu.VMEM((chunks, rows, WIDE), jnp.float32),
                pltpu.VMEM((2, chunks, 2, top, piece), jnp.bfloat16),
                pltpu.VMEM((2, chunks, 2, top, piece), jnp.bfloat16),
                pltpu.VMEM((2, chunks, top, piece), jnp.bfloat16),
                pltpu.VMEM((2, chunks, top, piece), jnp.bfloat16),
                dma((SLOTS, 2)),
                dma((3, XCUT)),
                dma((2, 1, chunks)),
                dma((2, 4, chunks)),
                dma((2, 4, chunks)),
            ],
            compiler_params=pltpu.CompilerParams(
                collective_id=0, has_side_effects=True, vmem_limit_bytes=64_000_000
            ),
        )(x, w_gate, w_up, w_down)

    return jax.shard_map(
        step,
        mesh=mesh,
        in_specs=(P("dp", None), P(None, "tp"), P(None, "tp"), P("tp", None)),
        out_specs=P("dp", None),
        check_vma=False,
    )
```

```python
import jax
import jax.numpy as jnp
from jax import lax
from jax.experimental import pallas as pl
from jax.experimental.pallas import tpu as pltpu
from jax.sharding import PartitionSpec as P

MESH = pl.DeviceIdType.MESH
SLOTS = 8
WIDE = 512
XCUT = 4
EARLY = 2
OWN = 1
ORDER = (
    "d0", "d1", "d2", "c0", "d3", "c1", "d4", "c2", "c3", "d5", "p0", "c4", "d6",
    "p1", "c5", "d7", "p2", "c6", "p3", "f0", "d8", "p4", "c7", "d9", "f2", "c8",
    "p6", "c9", "p5", "f3", "p7", "f4", "p8", "f1", "p9", "f6", "f5", "f7", "w3",
    "f8", "f9", "w4", "w6", "w0", "w1", "w5", "w2", "w7", "w8", "w9",
)


def kernel(x, wg, wu, wd, y, xs, h, slots, acc, dsend, drecv, s1, r1, s2, r2, wsem, xsem, rsem, out_sem):
    rows, d = x.shape
    half = wg.shape[1] // 2
    unit = WIDE // 2
    first = half % unit
    steps = half // unit + 1
    chunks = d // WIDE
    part_rows = rows // 4
    top = part_rows // 2

    dp, tp = lax.axis_index("dp"), lax.axis_index("tp")
    core = lax.rem(dp, 2)
    other = {"dp": dp + 1 - 2 * core}
    right_at, left_at, far_at = lax.rem(tp + 1, 4), lax.rem(tp + 3, 4), lax.rem(tp + 2, 4)
    sides = ({"tp": right_at}, {"tp": left_at})
    to_at, from_at = (right_at, left_at), (left_at, right_at)
    base = core * half

    def gate_up(step, width):
        slot = lax.rem(step, SLOTS)
        at = base if width == first else base + first + (step - 1) * unit
        cols = pl.ds(pl.multiple_of(at, 128), width)
        for k, w in enumerate((wg, wu)):
            pltpu.make_async_copy(w.at[:, cols], slots.at[slot, :, pl.ds(k * width, width)], wsem.at[slot]).start()

    def arrive(step, width):
        slot = lax.rem(step, SLOTS)
        both = slots.at[slot, :, pl.ds(0, 2 * width)]
        pltpu.make_async_copy(both, both, wsem.at[slot]).wait()

    def down(chunk):
        slot = lax.rem(chunk + steps, SLOTS)
        cols = pl.ds(pl.multiple_of(chunk * WIDE, 128), WIDE)
        return pltpu.make_async_copy(
            wd.at[pl.ds(pl.multiple_of(base, 128), half), cols], slots.at[slot, pl.ds(0, half), :], wsem.at[slot]
        )

    def refill(step):
        @pl.when(step < steps)
        def _():
            gate_up(step, unit)

        @pl.when(jnp.logical_and(step >= steps, step < steps + chunks))
        def _():
            down(step - steps).start()

    xw = d // XCUT
    ours, theirs, everyone = pl.ds(0, rows), pl.ds(rows, rows), pl.ds(0, 2 * rows)

    def x_in(k):
        cols = pl.ds(k * xw, xw)
        return pltpu.make_async_copy(x.at[:, cols], xs.at[ours, cols], xsem.at[2 + k])

    def x_out(cols):
        return pltpu.make_async_remote_copy(
            src_ref=xs.at[ours, cols], dst_ref=xs.at[theirs, cols], send_sem=xsem.at[0], recv_sem=xsem.at[1],
            device_id=other, device_id_type=MESH,
        )

    barrier = pltpu.get_barrier_semaphore()
    for who in (other, *sides):
        pl.semaphore_signal(barrier, inc=1, device_id=who, device_id_type=MESH)
    for k in range(XCUT):
        x_in(k).start()
    gate_up(0, first)
    for k in range(XCUT):
        x_in(k).wait()
    for s in range(1, EARLY):
        gate_up(s, unit)
    pl.semaphore_wait(barrier, 3)

    for k in range(XCUT):
        x_out(pl.ds(k * xw, xw)).start()
    for s in range(EARLY, SLOTS):
        gate_up(s, unit)

    def hidden(step, width, span):
        slot = lax.rem(step, SLOTS)
        at = 0 if width == first else pl.multiple_of(first + (step - 1) * unit, 128)
        both = jnp.dot(xs[span, :], slots[slot, :, : 2 * width], preferred_element_type=jnp.float32)
        h[span, pl.ds(at, width)] = (jax.nn.silu(both[:, :width]) * both[:, width:]).astype(h.dtype)

    arrive(0, first)
    hidden(0, first, ours)

    @pl.loop(1, OWN)
    def _(s):
        arrive(s, unit)
        hidden(s, unit, ours)

    x_out(pl.ds(0, d)).wait_recv()
    hidden(0, first, theirs)
    refill(SLOTS)

    @pl.loop(1, OWN)
    def _(s):
        hidden(s, unit, theirs)
        refill(s + SLOTS)

    @pl.loop(OWN, steps)
    def _(s):
        arrive(s, unit)
        hidden(s, unit, everyone)
        refill(s + SLOTS)

    def send(src, dst, kind, j, who):
        return pltpu.make_async_remote_copy(
            src_ref=src, dst_ref=dst, send_sem=out_sem.at[kind], recv_sem=rsem.at[kind, j], device_id=who,
            device_id_type=MESH,
        )

    def cols_of(j):
        return pl.ds(j * WIDE, WIDE)

    def got(ref, kind, j):
        pltpu.make_async_copy(ref, ref, rsem.at[kind, j]).wait()

    def place(at, k=None):
        if k is None:
            return pl.ds(pl.multiple_of(at * part_rows, part_rows), part_rows)
        return pl.ds(pl.multiple_of(at * part_rows + k * top, top), top)

    def matmul(j):
        slot = (j + steps) % SLOTS
        down(j).wait()
        out = jnp.dot(h[...], slots[slot, :half, :], preferred_element_type=jnp.float32)
        acc[:, cols_of(j)] = out[:rows]
        dsend[:, cols_of(j)] = out[rows:].astype(dsend.dtype)
        send(dsend.at[:, cols_of(j)], drecv.at[:, cols_of(j)], 0, j, other).start()
        if j + SLOTS < chunks:
            down(j + SLOTS).start()

    def chip_sum(j):
        cols = cols_of(j)
        got(drecv.at[:, cols], 0, j)
        acc[:, cols] += drecv[:, cols].astype(jnp.float32)
        for k in range(2):
            s1[k, 0, :, cols] = acc[place(far_at, k), cols].astype(s1.dtype)
            s1[k, 1, :, cols] = acc[place(to_at[k], 1 - k), cols].astype(s1.dtype)
            send(s1.at[k, :, :, cols], r1.at[k, :, :, cols], 1, j, sides[k]).start()

    def second(j):
        cols = cols_of(j)
        got(r1.at[:, :, :, cols], 1, j)
        for k in range(2):
            s2[k, :, cols] = (acc[place(to_at[k], k), cols] + r1[k, 0, :, cols].astype(jnp.float32)).astype(s2.dtype)
            send(s2.at[k, :, cols], r2.at[k, :, cols], 2, j, sides[k]).start()

    def finish(j):
        cols = cols_of(j)
        got(r2.at[:, :, cols], 2, j)
        for k in range(2):
            total = acc[place(tp, k), cols] + r2[k, :, cols].astype(jnp.float32) + r1[1 - k, 1, :, cols].astype(jnp.float32)
            y[place(tp, k), cols] = total.astype(y.dtype)
        for k in range(2):
            mine = y.at[place(tp), cols]
            send(mine, mine, 3, j, sides[k]).start()

    def pass_on(j):
        cols = cols_of(j)
        got(y.at[pl.ds(0, 2 * part_rows), cols], 3, j)
        for k in range(2):
            piece = y.at[place(from_at[k], k), cols]
            send(piece, piece, 4, j, sides[k]).start()

    does = {"d": matmul, "c": chip_sum, "p": second, "f": finish, "w": pass_on}
    assert sorted(ORDER) == sorted(op + str(j) for op in does for j in range(chunks))
    for token in ORDER:
        does[token[0]](int(token[1:]))
    for j in range(chunks):
        got(y.at[pl.ds(0, part_rows), cols_of(j)], 4, j)

    x_out(pl.ds(0, d)).wait_send()
    for kind, ref in enumerate((dsend, s1, s2, y.at[pl.ds(0, 2 * part_rows), :], y.at[pl.ds(0, part_rows), :])):
        pltpu.make_async_copy(ref, ref, out_sem.at[kind]).wait()


def solution(mesh):
    assert mesh.shape["tp"] == 4 and mesh.shape["dp"] % 2 == 0

    def step(x, w_gate, w_up, w_down):
        rows, d = x.shape
        half = w_gate.shape[1] // 2
        chunks, top = d // WIDE, rows // 8
        dma = pltpu.SemaphoreType.DMA
        return pl.pallas_call(
            kernel,
            out_shape=pltpu.VMEM((rows, d), jnp.bfloat16),
            in_specs=[pl.BlockSpec(memory_space=pl.ANY)] * 4,
            out_specs=pl.BlockSpec(memory_space=pltpu.VMEM),
            scratch_shapes=[
                pltpu.VMEM((2 * rows, d), jnp.bfloat16),
                pltpu.VMEM((2 * rows, half), jnp.bfloat16),
                pltpu.VMEM((SLOTS, d, WIDE), jnp.bfloat16),
                pltpu.VMEM((rows, d), jnp.float32),
                pltpu.VMEM((rows, d), jnp.bfloat16),
                pltpu.VMEM((rows, d), jnp.bfloat16),
                pltpu.VMEM((2, 2, top, d), jnp.bfloat16),
                pltpu.VMEM((2, 2, top, d), jnp.bfloat16),
                pltpu.VMEM((2, top, d), jnp.bfloat16),
                pltpu.VMEM((2, top, d), jnp.bfloat16),
                dma((SLOTS,)),
                dma((2 + XCUT,)),
                dma((5, chunks)),
                dma((5,)),
            ],
            compiler_params=pltpu.CompilerParams(
                collective_id=0, has_side_effects=True, vmem_limit_bytes=64_000_000
            ),
        )(x, w_gate, w_up, w_down)

    return jax.shard_map(
        step,
        mesh=mesh,
        in_specs=(P("dp", None), P(None, "tp"), P(None, "tp"), P("tp", None)),
        out_specs=P("dp", None),
        check_vma=False,
    )
```

```python
import jax
import jax.numpy as jnp
from jax import lax
from jax.experimental import pallas as pl
from jax.experimental.pallas import tpu as pltpu
from jax.sharding import PartitionSpec as P

MESH = pl.DeviceIdType.MESH
SLOTS = 8
WIDE = 512
XCUT = 4
OWN = 1
ORDER = (
    "d0", "d1", "d2", "c0", "d3", "c1", "c2", "d4", "c3", "d5", "p0", "c4", "d6",
    "p1", "c5", "d7", "p2", "c6", "p3", "d8", "c7", "f0", "d9", "f1", "c8", "c9",
    "p5", "p6", "f2", "p4", "p7", "f3", "p8", "p9", "f5", "f6", "f4", "f7", "f8",
    "f9", "w3", "w0", "w5", "w4", "w2", "w1", "w7", "w8", "w6", "w9",
)


def kernel(x, wg, wu, wd, y, xs, h, slots, acc, dsend, drecv, s1, r1, s2, r2, wsem, xsem, rsem, out_sem):
    rows, d = x.shape
    half = wg.shape[1] // 2
    unit = WIDE // 2
    first = half % unit
    steps = half // unit + 1
    chunks = d // WIDE
    part_rows = rows // 4
    top = part_rows // 2

    dp, tp = lax.axis_index("dp"), lax.axis_index("tp")
    core = lax.rem(dp, 2)
    other = {"dp": dp + 1 - 2 * core}
    right_at, left_at, far_at = lax.rem(tp + 1, 4), lax.rem(tp + 3, 4), lax.rem(tp + 2, 4)
    sides = ({"tp": right_at}, {"tp": left_at})
    to_at, from_at = (right_at, left_at), (left_at, right_at)
    base = core * half

    def gate_up(step, width):
        slot = lax.rem(step, SLOTS)
        at = base if width == first else base + first + (step - 1) * unit
        cols = pl.ds(pl.multiple_of(at, 128), width)
        for k, w in enumerate((wg, wu)):
            pltpu.make_async_copy(w.at[:, cols], slots.at[slot, :, pl.ds(k * width, width)], wsem.at[slot]).start()

    def arrive(step, width):
        slot = lax.rem(step, SLOTS)
        both = slots.at[slot, :, pl.ds(0, 2 * width)]
        pltpu.make_async_copy(both, both, wsem.at[slot]).wait()

    def down(chunk):
        slot = lax.rem(chunk + steps, SLOTS)
        cols = pl.ds(pl.multiple_of(chunk * WIDE, 128), WIDE)
        return pltpu.make_async_copy(
            wd.at[pl.ds(pl.multiple_of(base, 128), half), cols], slots.at[slot, pl.ds(0, half), :], wsem.at[slot]
        )

    def refill(step):
        @pl.when(step < steps)
        def _():
            gate_up(step, unit)

        @pl.when(jnp.logical_and(step >= steps, step < steps + chunks))
        def _():
            down(step - steps).start()

    xw = d // XCUT
    ours, theirs, everyone = pl.ds(0, rows), pl.ds(rows, rows), pl.ds(0, 2 * rows)

    def x_in(k):
        cols = pl.ds(k * xw, xw)
        return pltpu.make_async_copy(x.at[:, cols], xs.at[ours, cols], xsem.at[2 + k])

    def x_out(cols):
        return pltpu.make_async_remote_copy(
            src_ref=xs.at[ours, cols], dst_ref=xs.at[theirs, cols], send_sem=xsem.at[0], recv_sem=xsem.at[1],
            device_id=other, device_id_type=MESH,
        )

    barrier = pltpu.get_barrier_semaphore()
    for who in (other, *sides):
        pl.semaphore_signal(barrier, inc=1, device_id=who, device_id_type=MESH)
    for k in range(XCUT):
        x_in(k).start()
    gate_up(0, first)
    pl.semaphore_wait(barrier, 3)

    for k in range(XCUT):
        x_in(k).wait()
        x_out(pl.ds(k * xw, xw)).start()
    for s in range(1, SLOTS):
        gate_up(s, unit)

    def hidden(step, width, span):
        slot = lax.rem(step, SLOTS)
        at = 0 if width == first else pl.multiple_of(first + (step - 1) * unit, 128)
        both = jnp.dot(xs[span, :], slots[slot, :, : 2 * width], preferred_element_type=jnp.float32)
        h[span, pl.ds(at, width)] = (jax.nn.silu(both[:, :width]) * both[:, width:]).astype(h.dtype)

    arrive(0, first)
    hidden(0, first, ours)

    @pl.loop(1, OWN)
    def _(s):
        arrive(s, unit)
        hidden(s, unit, ours)

    x_out(pl.ds(0, d)).wait_recv()
    hidden(0, first, theirs)
    refill(SLOTS)

    @pl.loop(1, OWN)
    def _(s):
        hidden(s, unit, theirs)
        refill(s + SLOTS)

    @pl.loop(OWN, steps)
    def _(s):
        arrive(s, unit)
        hidden(s, unit, everyone)
        refill(s + SLOTS)

    def send(src, dst, kind, j, who):
        return pltpu.make_async_remote_copy(
            src_ref=src, dst_ref=dst, send_sem=out_sem.at[kind], recv_sem=rsem.at[kind, j], device_id=who,
            device_id_type=MESH,
        )

    def cols_of(j):
        return pl.ds(j * WIDE, WIDE)

    def got(ref, kind, j):
        pltpu.make_async_copy(ref, ref, rsem.at[kind, j]).wait()

    def place(at, k=None):
        if k is None:
            return pl.ds(pl.multiple_of(at * part_rows, part_rows), part_rows)
        return pl.ds(pl.multiple_of(at * part_rows + k * top, top), top)

    def matmul(j):
        slot = (j + steps) % SLOTS
        down(j).wait()
        out = jnp.dot(h[...], slots[slot, :half, :], preferred_element_type=jnp.float32)
        acc[:, cols_of(j)] = out[:rows]
        dsend[:, cols_of(j)] = out[rows:].astype(dsend.dtype)
        send(dsend.at[:, cols_of(j)], drecv.at[:, cols_of(j)], 0, j, other).start()
        if j + SLOTS < chunks:
            down(j + SLOTS).start()

    def chip_sum(j):
        cols = cols_of(j)
        got(drecv.at[:, cols], 0, j)
        acc[:, cols] += drecv[:, cols].astype(jnp.float32)
        for k in range(2):
            s1[k, 0, :, cols] = acc[place(far_at, k), cols].astype(s1.dtype)
            s1[k, 1, :, cols] = acc[place(to_at[k], 1 - k), cols].astype(s1.dtype)
            send(s1.at[k, :, :, cols], r1.at[k, :, :, cols], 1, j, sides[k]).start()

    def second(j):
        cols = cols_of(j)
        got(r1.at[:, :, :, cols], 1, j)
        for k in range(2):
            s2[k, :, cols] = (acc[place(to_at[k], k), cols] + r1[k, 0, :, cols].astype(jnp.float32)).astype(s2.dtype)
            send(s2.at[k, :, cols], r2.at[k, :, cols], 2, j, sides[k]).start()

    def finish(j):
        cols = cols_of(j)
        got(r2.at[:, :, cols], 2, j)
        for k in range(2):
            total = acc[place(tp, k), cols] + r2[k, :, cols].astype(jnp.float32) + r1[1 - k, 1, :, cols].astype(jnp.float32)
            y[place(tp, k), cols] = total.astype(y.dtype)
        for k in range(2):
            mine = y.at[place(tp), cols]
            send(mine, mine, 3, j, sides[k]).start()

    def pass_on(j):
        cols = cols_of(j)
        got(y.at[pl.ds(0, 2 * part_rows), cols], 3, j)
        for k in range(2):
            piece = y.at[place(from_at[k], k), cols]
            send(piece, piece, 4, j, sides[k]).start()

    does = {"d": matmul, "c": chip_sum, "p": second, "f": finish, "w": pass_on}
    assert sorted(ORDER) == sorted(op + str(j) for op in does for j in range(chunks))
    for token in ORDER:
        does[token[0]](int(token[1:]))
    for j in range(chunks):
        got(y.at[pl.ds(0, part_rows), cols_of(j)], 4, j)

    x_out(pl.ds(0, d)).wait_send()
    for kind, ref in enumerate((dsend, s1, s2, y.at[pl.ds(0, 2 * part_rows), :], y.at[pl.ds(0, part_rows), :])):
        pltpu.make_async_copy(ref, ref, out_sem.at[kind]).wait()


def solution(mesh):
    assert mesh.shape["tp"] == 4 and mesh.shape["dp"] % 2 == 0

    def step(x, w_gate, w_up, w_down):
        rows, d = x.shape
        half = w_gate.shape[1] // 2
        chunks, top = d // WIDE, rows // 8
        dma = pltpu.SemaphoreType.DMA
        return pl.pallas_call(
            kernel,
            out_shape=pltpu.VMEM((rows, d), jnp.bfloat16),
            in_specs=[pl.BlockSpec(memory_space=pl.ANY)] * 4,
            out_specs=pl.BlockSpec(memory_space=pltpu.VMEM),
            scratch_shapes=[
                pltpu.VMEM((2 * rows, d), jnp.bfloat16),
                pltpu.VMEM((2 * rows, half), jnp.bfloat16),
                pltpu.VMEM((SLOTS, d, WIDE), jnp.bfloat16),
                pltpu.VMEM((rows, d), jnp.float32),
                pltpu.VMEM((rows, d), jnp.bfloat16),
                pltpu.VMEM((rows, d), jnp.bfloat16),
                pltpu.VMEM((2, 2, top, d), jnp.bfloat16),
                pltpu.VMEM((2, 2, top, d), jnp.bfloat16),
                pltpu.VMEM((2, top, d), jnp.bfloat16),
                pltpu.VMEM((2, top, d), jnp.bfloat16),
                dma((SLOTS,)),
                dma((2 + XCUT,)),
                dma((5, chunks)),
                dma((5,)),
            ],
            compiler_params=pltpu.CompilerParams(
                collective_id=0, has_side_effects=True, vmem_limit_bytes=64_000_000
            ),
        )(x, w_gate, w_up, w_down)

    return jax.shard_map(
        step,
        mesh=mesh,
        in_specs=(P("dp", None), P(None, "tp"), P(None, "tp"), P("tp", None)),
        out_specs=P("dp", None),
        check_vma=False,
    )
```

```python
import jax
import jax.numpy as jnp
from jax import lax
from jax.experimental import pallas as pl
from jax.experimental.pallas import tpu as pltpu
from jax.sharding import PartitionSpec as P

MESH = pl.DeviceIdType.MESH
SLOTS = 8
WIDE = 512
XCUT = 4
OWN = 1
ORDER = (
    "d0", "d1", "c0", "d2", "c1", "d3", "c2", "d4", "c3", "p0", "d5", "c4", "p1",
    "d6", "c5", "p2", "d7", "p3", "c6", "f0", "d8", "c7", "p4", "d9", "c8", "p5",
    "c9", "f3", "p6", "p7", "f4", "p8", "f1", "p9", "f5", "f6", "f2", "f8", "f7",
    "f9", "w4", "w5", "w1", "w2", "w0", "w8", "w3", "w6", "w7", "w9",
)


def kernel(x, wg, wu, wd, y, xs, h, slots, acc, dsend, drecv, s1, r1, s2, r2, wsem, xsem, rsem, out_sem):
    rows, d = x.shape
    half = wg.shape[1] // 2
    unit = WIDE // 2
    first = half % unit
    steps = half // unit + 1
    chunks = d // WIDE
    part_rows = rows // 4
    top = part_rows // 2

    dp, tp = lax.axis_index("dp"), lax.axis_index("tp")
    core = lax.rem(dp, 2)
    other = {"dp": dp + 1 - 2 * core}
    right_at, left_at, far_at = lax.rem(tp + 1, 4), lax.rem(tp + 3, 4), lax.rem(tp + 2, 4)
    sides = ({"tp": right_at}, {"tp": left_at})
    to_at, from_at = (right_at, left_at), (left_at, right_at)
    base = core * half

    def gate_up(step, width):
        slot = lax.rem(step, SLOTS)
        at = base if width == first else base + first + (step - 1) * unit
        cols = pl.ds(pl.multiple_of(at, 128), width)
        for k, w in enumerate((wg, wu)):
            pltpu.make_async_copy(w.at[:, cols], slots.at[slot, :, pl.ds(k * width, width)], wsem.at[slot]).start()

    def arrive(step, width):
        slot = lax.rem(step, SLOTS)
        both = slots.at[slot, :, pl.ds(0, 2 * width)]
        pltpu.make_async_copy(both, both, wsem.at[slot]).wait()

    def down(chunk):
        slot = lax.rem(chunk + steps, SLOTS)
        cols = pl.ds(pl.multiple_of(chunk * WIDE, 128), WIDE)
        return pltpu.make_async_copy(
            wd.at[pl.ds(pl.multiple_of(base, 128), half), cols], slots.at[slot, pl.ds(0, half), :], wsem.at[slot]
        )

    def refill(step):
        @pl.when(step < steps)
        def _():
            gate_up(step, unit)

        @pl.when(jnp.logical_and(step >= steps, step < steps + chunks))
        def _():
            down(step - steps).start()

    xw = d // XCUT
    ours, theirs, everyone = pl.ds(0, rows), pl.ds(rows, rows), pl.ds(0, 2 * rows)

    def x_in(k):
        cols = pl.ds(k * xw, xw)
        return pltpu.make_async_copy(x.at[:, cols], xs.at[ours, cols], xsem.at[2 + k])

    def x_out(cols):
        return pltpu.make_async_remote_copy(
            src_ref=xs.at[ours, cols], dst_ref=xs.at[theirs, cols], send_sem=xsem.at[0], recv_sem=xsem.at[1],
            device_id=other, device_id_type=MESH,
        )

    barrier = pltpu.get_barrier_semaphore()
    for who in (other, *sides):
        pl.semaphore_signal(barrier, inc=1, device_id=who, device_id_type=MESH)
    for k in range(XCUT):
        x_in(k).start()
    for k in range(XCUT):
        x_in(k).wait()
    gate_up(0, first)
    pl.semaphore_wait(barrier, 3)

    for k in range(XCUT):
        x_out(pl.ds(k * xw, xw)).start()
    for s in range(1, SLOTS):
        gate_up(s, unit)

    def hidden(step, width, span):
        slot = lax.rem(step, SLOTS)
        at = 0 if width == first else pl.multiple_of(first + (step - 1) * unit, 128)
        both = jnp.dot(xs[span, :], slots[slot, :, : 2 * width], preferred_element_type=jnp.float32)
        h[span, pl.ds(at, width)] = (jax.nn.silu(both[:, :width]) * both[:, width:]).astype(h.dtype)

    arrive(0, first)
    hidden(0, first, ours)

    @pl.loop(1, OWN)
    def _(s):
        arrive(s, unit)
        hidden(s, unit, ours)

    x_out(pl.ds(0, d)).wait_recv()
    hidden(0, first, theirs)
    refill(SLOTS)

    @pl.loop(1, OWN)
    def _(s):
        hidden(s, unit, theirs)
        refill(s + SLOTS)

    @pl.loop(OWN, steps)
    def _(s):
        arrive(s, unit)
        hidden(s, unit, everyone)
        refill(s + SLOTS)

    def send(src, dst, kind, j, who):
        return pltpu.make_async_remote_copy(
            src_ref=src, dst_ref=dst, send_sem=out_sem.at[kind], recv_sem=rsem.at[kind, j], device_id=who,
            device_id_type=MESH,
        )

    def cols_of(j):
        return pl.ds(j * WIDE, WIDE)

    def got(ref, kind, j):
        pltpu.make_async_copy(ref, ref, rsem.at[kind, j]).wait()

    def place(at, k=None):
        if k is None:
            return pl.ds(pl.multiple_of(at * part_rows, part_rows), part_rows)
        return pl.ds(pl.multiple_of(at * part_rows + k * top, top), top)

    def matmul(j):
        slot = (j + steps) % SLOTS
        down(j).wait()
        out = jnp.dot(h[...], slots[slot, :half, :], preferred_element_type=jnp.float32)
        acc[:, cols_of(j)] = out[:rows]
        dsend[:, cols_of(j)] = out[rows:].astype(dsend.dtype)
        send(dsend.at[:, cols_of(j)], drecv.at[:, cols_of(j)], 0, j, other).start()
        if j + SLOTS < chunks:
            down(j + SLOTS).start()

    def chip_sum(j):
        cols = cols_of(j)
        got(drecv.at[:, cols], 0, j)
        acc[:, cols] += drecv[:, cols].astype(jnp.float32)
        for k in range(2):
            s1[k, 0, :, cols] = acc[place(far_at, k), cols].astype(s1.dtype)
            s1[k, 1, :, cols] = acc[place(to_at[k], 1 - k), cols].astype(s1.dtype)
            send(s1.at[k, :, :, cols], r1.at[k, :, :, cols], 1, j, sides[k]).start()

    def second(j):
        cols = cols_of(j)
        got(r1.at[:, :, :, cols], 1, j)
        for k in range(2):
            s2[k, :, cols] = (acc[place(to_at[k], k), cols] + r1[k, 0, :, cols].astype(jnp.float32)).astype(s2.dtype)
            send(s2.at[k, :, cols], r2.at[k, :, cols], 2, j, sides[k]).start()

    def finish(j):
        cols = cols_of(j)
        got(r2.at[:, :, cols], 2, j)
        for k in range(2):
            total = acc[place(tp, k), cols] + r2[k, :, cols].astype(jnp.float32) + r1[1 - k, 1, :, cols].astype(jnp.float32)
            y[place(tp, k), cols] = total.astype(y.dtype)
        for k in range(2):
            mine = y.at[place(tp), cols]
            send(mine, mine, 3, j, sides[k]).start()

    def pass_on(j):
        cols = cols_of(j)
        got(y.at[pl.ds(0, 2 * part_rows), cols], 3, j)
        for k in range(2):
            piece = y.at[place(from_at[k], k), cols]
            send(piece, piece, 4, j, sides[k]).start()

    does = {"d": matmul, "c": chip_sum, "p": second, "f": finish, "w": pass_on}
    assert sorted(ORDER) == sorted(op + str(j) for op in does for j in range(chunks))
    for token in ORDER:
        does[token[0]](int(token[1:]))
    for j in range(chunks):
        got(y.at[pl.ds(0, part_rows), cols_of(j)], 4, j)

    x_out(pl.ds(0, d)).wait_send()
    for kind, ref in enumerate((dsend, s1, s2, y.at[pl.ds(0, 2 * part_rows), :], y.at[pl.ds(0, part_rows), :])):
        pltpu.make_async_copy(ref, ref, out_sem.at[kind]).wait()


def solution(mesh):
    assert mesh.shape["tp"] == 4 and mesh.shape["dp"] % 2 == 0

    def step(x, w_gate, w_up, w_down):
        rows, d = x.shape
        half = w_gate.shape[1] // 2
        chunks, top = d // WIDE, rows // 8
        dma = pltpu.SemaphoreType.DMA
        return pl.pallas_call(
            kernel,
            out_shape=pltpu.VMEM((rows, d), jnp.bfloat16),
            in_specs=[pl.BlockSpec(memory_space=pl.ANY)] * 4,
            out_specs=pl.BlockSpec(memory_space=pltpu.VMEM),
            scratch_shapes=[
                pltpu.VMEM((2 * rows, d), jnp.bfloat16),
                pltpu.VMEM((2 * rows, half), jnp.bfloat16),
                pltpu.VMEM((SLOTS, d, WIDE), jnp.bfloat16),
                pltpu.VMEM((rows, d), jnp.float32),
                pltpu.VMEM((rows, d), jnp.bfloat16),
                pltpu.VMEM((rows, d), jnp.bfloat16),
                pltpu.VMEM((2, 2, top, d), jnp.bfloat16),
                pltpu.VMEM((2, 2, top, d), jnp.bfloat16),
                pltpu.VMEM((2, top, d), jnp.bfloat16),
                pltpu.VMEM((2, top, d), jnp.bfloat16),
                dma((SLOTS,)),
                dma((2 + XCUT,)),
                dma((5, chunks)),
                dma((5,)),
            ],
            compiler_params=pltpu.CompilerParams(
                collective_id=0, has_side_effects=True, vmem_limit_bytes=64_000_000
            ),
        )(x, w_gate, w_up, w_down)

    return jax.shard_map(
        step,
        mesh=mesh,
        in_specs=(P("dp", None), P(None, "tp"), P(None, "tp"), P("tp", None)),
        out_specs=P("dp", None),
        check_vma=False,
    )
```

```python
import jax
import jax.numpy as jnp
from jax import lax
from jax.experimental import pallas as pl
from jax.experimental.pallas import tpu as pltpu
from jax.sharding import PartitionSpec as P

MESH = pl.DeviceIdType.MESH
SLOTS = 8
WIDE = 512
XCUT = 4
OWN = 1
ORDER = (
    "d0", "d1", "c0", "d2", "c1", "d3", "c2", "d4", "c3", "p0", "d5", "c4", "p1",
    "d6", "c5", "p2", "d7", "p3", "c6", "f0", "d8", "c7", "p4", "d9", "c8", "p5",
    "c9", "f3", "p6", "p7", "f4", "p8", "f1", "p9", "f5", "f6", "f2", "f8", "f7",
    "f9", "w4", "w5", "w1", "w2", "w0", "w8", "w3", "w6", "w7", "w9",
)


def kernel(x, wg, wu, wd, y, xs, h, slots, acc, dsend, drecv, s1, r1, s2, r2, wsem, xsem, rsem, out_sem):
    rows, d = x.shape
    half = wg.shape[1] // 2
    unit = WIDE // 2
    first = half % unit
    steps = half // unit + 1
    chunks = d // WIDE
    part_rows = rows // 4
    top = part_rows // 2

    dp, tp = lax.axis_index("dp"), lax.axis_index("tp")
    core = lax.rem(dp, 2)
    other = {"dp": dp + 1 - 2 * core}
    right_at, left_at, far_at = lax.rem(tp + 1, 4), lax.rem(tp + 3, 4), lax.rem(tp + 2, 4)
    sides = ({"tp": right_at}, {"tp": left_at})
    to_at, from_at = (right_at, left_at), (left_at, right_at)
    base = core * half

    def gate_up(step, width):
        slot = lax.rem(step, SLOTS)
        at = base if width == first else base + first + (step - 1) * unit
        cols = pl.ds(pl.multiple_of(at, 128), width)
        for k, w in enumerate((wg, wu)):
            pltpu.make_async_copy(w.at[:, cols], slots.at[slot, :, pl.ds(k * width, width)], wsem.at[slot]).start()

    def arrive(step, width):
        slot = lax.rem(step, SLOTS)
        both = slots.at[slot, :, pl.ds(0, 2 * width)]
        pltpu.make_async_copy(both, both, wsem.at[slot]).wait()

    def down(chunk):
        slot = lax.rem(chunk + steps, SLOTS)
        cols = pl.ds(pl.multiple_of(chunk * WIDE, 128), WIDE)
        return pltpu.make_async_copy(
            wd.at[pl.ds(pl.multiple_of(base, 128), half), cols], slots.at[slot, pl.ds(0, half), :], wsem.at[slot]
        )

    def refill(step):
        @pl.when(step < steps)
        def _():
            gate_up(step, unit)

        @pl.when(jnp.logical_and(step >= steps, step < steps + chunks))
        def _():
            down(step - steps).start()

    xw = d // XCUT
    ours, theirs, everyone = pl.ds(0, rows), pl.ds(rows, rows), pl.ds(0, 2 * rows)

    def x_in(k):
        cols = pl.ds(k * xw, xw)
        return pltpu.make_async_copy(x.at[:, cols], xs.at[ours, cols], xsem.at[2 + k])

    def x_out(cols):
        return pltpu.make_async_remote_copy(
            src_ref=xs.at[ours, cols], dst_ref=xs.at[theirs, cols], send_sem=xsem.at[0], recv_sem=xsem.at[1],
            device_id=other, device_id_type=MESH,
        )

    barrier = pltpu.get_barrier_semaphore()
    for who in (other, *sides):
        pl.semaphore_signal(barrier, inc=1, device_id=who, device_id_type=MESH)
    for k in range(XCUT):
        x_in(k).start()
    for k in range(XCUT):
        x_in(k).wait()
    gate_up(0, first)
    pl.semaphore_wait(barrier, 3)

    for k in range(XCUT):
        x_out(pl.ds(k * xw, xw)).start()
    for s in range(1, SLOTS):
        gate_up(s, unit)

    def hidden(step, width, span):
        slot = lax.rem(step, SLOTS)
        at = 0 if width == first else pl.multiple_of(first + (step - 1) * unit, 128)
        both = jnp.dot(xs[span, :], slots[slot, :, : 2 * width], preferred_element_type=jnp.float32)
        h[span, pl.ds(at, width)] = (jax.nn.silu(both[:, :width]) * both[:, width:]).astype(h.dtype)

    arrive(0, first)
    hidden(0, first, ours)

    @pl.loop(1, OWN)
    def _(s):
        arrive(s, unit)
        hidden(s, unit, ours)

    x_out(pl.ds(0, d)).wait_recv()
    hidden(0, first, theirs)
    refill(SLOTS)

    @pl.loop(1, OWN)
    def _(s):
        hidden(s, unit, theirs)
        refill(s + SLOTS)

    @pl.loop(OWN, steps)
    def _(s):
        arrive(s, unit)
        hidden(s, unit, everyone)
        refill(s + SLOTS)

    def send(src, dst, kind, j, who):
        return pltpu.make_async_remote_copy(
            src_ref=src, dst_ref=dst, send_sem=out_sem.at[kind], recv_sem=rsem.at[kind, j], device_id=who,
            device_id_type=MESH,
        )

    def cols_of(j):
        return pl.ds(j * WIDE, WIDE)

    def got(ref, kind, j):
        pltpu.make_async_copy(ref, ref, rsem.at[kind, j]).wait()

    def place(at, k=None):
        if k is None:
            return pl.ds(pl.multiple_of(at * part_rows, part_rows), part_rows)
        return pl.ds(pl.multiple_of(at * part_rows + k * top, top), top)

    def matmul(j):
        slot = (j + steps) % SLOTS
        down(j).wait()
        out = jnp.dot(h[...], slots[slot, :half, :], preferred_element_type=jnp.float32)
        acc[:, cols_of(j)] = out[:rows]
        dsend[:, cols_of(j)] = out[rows:].astype(dsend.dtype)
        send(dsend.at[:, cols_of(j)], drecv.at[:, cols_of(j)], 0, j, other).start()
        if j + SLOTS < chunks:
            down(j + SLOTS).start()

    def chip_sum(j):
        cols = cols_of(j)
        got(drecv.at[:, cols], 0, j)
        acc[:, cols] += drecv[:, cols].astype(jnp.float32)
        for k in range(2):
            s1[k, 0, :, cols] = acc[place(far_at, k), cols].astype(s1.dtype)
            send(s1.at[k, 0, :, cols], r1.at[k, 0, :, cols], 1, j, sides[k]).start()
        for k in range(2):
            s1[k, 1, :, cols] = acc[place(to_at[k], 1 - k), cols].astype(s1.dtype)
            send(s1.at[k, 1, :, cols], r1.at[k, 1, :, cols], 5, j, sides[k]).start()

    def second(j):
        cols = cols_of(j)
        got(r1.at[:, 0, :, cols], 1, j)
        for k in range(2):
            s2[k, :, cols] = (acc[place(to_at[k], k), cols] + r1[k, 0, :, cols].astype(jnp.float32)).astype(s2.dtype)
            send(s2.at[k, :, cols], r2.at[k, :, cols], 2, j, sides[k]).start()

    def finish(j):
        cols = cols_of(j)
        got(r2.at[:, :, cols], 2, j)
        got(r1.at[:, 1, :, cols], 5, j)
        for k in range(2):
            total = acc[place(tp, k), cols] + r2[k, :, cols].astype(jnp.float32) + r1[1 - k, 1, :, cols].astype(jnp.float32)
            y[place(tp, k), cols] = total.astype(y.dtype)
        for k in range(2):
            mine = y.at[place(tp), cols]
            send(mine, mine, 3, j, sides[k]).start()

    def pass_on(j):
        cols = cols_of(j)
        got(y.at[pl.ds(0, 2 * part_rows), cols], 3, j)
        for k in range(2):
            piece = y.at[place(from_at[k], k), cols]
            send(piece, piece, 4, j, sides[k]).start()

    does = {"d": matmul, "c": chip_sum, "p": second, "f": finish, "w": pass_on}
    assert sorted(ORDER) == sorted(op + str(j) for op in does for j in range(chunks))
    for token in ORDER:
        does[token[0]](int(token[1:]))
    for j in range(chunks):
        got(y.at[pl.ds(0, part_rows), cols_of(j)], 4, j)

    x_out(pl.ds(0, d)).wait_send()
    for kind, ref in enumerate((dsend, s2, s2, y.at[pl.ds(0, 2 * part_rows), :], s2, s2)):
        pltpu.make_async_copy(ref, ref, out_sem.at[kind]).wait()


def solution(mesh):
    assert mesh.shape["tp"] == 4 and mesh.shape["dp"] % 2 == 0

    def step(x, w_gate, w_up, w_down):
        rows, d = x.shape
        half = w_gate.shape[1] // 2
        chunks, top = d // WIDE, rows // 8
        dma = pltpu.SemaphoreType.DMA
        return pl.pallas_call(
            kernel,
            out_shape=pltpu.VMEM((rows, d), jnp.bfloat16),
            in_specs=[pl.BlockSpec(memory_space=pl.ANY)] * 4,
            out_specs=pl.BlockSpec(memory_space=pltpu.VMEM),
            scratch_shapes=[
                pltpu.VMEM((2 * rows, d), jnp.bfloat16),
                pltpu.VMEM((2 * rows, half), jnp.bfloat16),
                pltpu.VMEM((SLOTS, d, WIDE), jnp.bfloat16),
                pltpu.VMEM((rows, d), jnp.float32),
                pltpu.VMEM((rows, d), jnp.bfloat16),
                pltpu.VMEM((rows, d), jnp.bfloat16),
                pltpu.VMEM((2, 2, top, d), jnp.bfloat16),
                pltpu.VMEM((2, 2, top, d), jnp.bfloat16),
                pltpu.VMEM((2, top, d), jnp.bfloat16),
                pltpu.VMEM((2, top, d), jnp.bfloat16),
                dma((SLOTS,)),
                dma((2 + XCUT,)),
                dma((6, chunks)),
                dma((6,)),
            ],
            compiler_params=pltpu.CompilerParams(
                collective_id=0, has_side_effects=True, vmem_limit_bytes=64_000_000
            ),
        )(x, w_gate, w_up, w_down)

    return jax.shard_map(
        step,
        mesh=mesh,
        in_specs=(P("dp", None), P(None, "tp"), P(None, "tp"), P("tp", None)),
        out_specs=P("dp", None),
        check_vma=False,
    )
```
